32 devices in a mesh: tp: 4 (over z), dp: 8 (over y, x, core).
Axes of the slice: x: 2, y: 2, z: 4, core: 2. Of those that a mesh axis runs over, the one named last changes fastest.
Arguments:
- tokens: int32 [8, 1024], P('dp')
- labels: int32 [8, 1024], P('dp')
- embedding: float32 [50304, 768], P('tp')
- vec_params: float32 [16, 768], replicated
- w_qkv: float32 [2, 768, 2304], P(None, None, 'tp')
- b_qkv: float32 [2, 12, 192], P(None, 'tp')
- w_out: float32 [2, 768, 768], P(None, 'tp')
- w_up: float32 [2, 768, 3072], P(None, None, 'tp')
- b_up: float32 [2, 3072], P(None, 'tp')
- w_down: float32 [2, 3072, 768], P(None, 'tp')
- mom_embedding: float32 [50304, 768], P('tp')
- mom_vec_params: float32 [16, 768], replicated
- mom_w_qkv: float32 [2, 768, 2304], P(None, None, 'tp')
- mom_b_qkv: float32 [2, 12, 192], P(None, 'tp')
- mom_w_out: float32 [2, 768, 768], P(None, 'tp')
- mom_w_up: float32 [2, 768, 3072], P(None, None, 'tp')
- mom_b_up: float32 [2, 3072], P(None, 'tp')
- mom_w_down: float32 [2, 3072, 768], P(None, 'tp')
- vel_embedding: float32 [50304, 768], P('tp')
- vel_vec_params: float32 [16, 768], replicated
- vel_w_qkv: float32 [2, 768, 2304], P(None, None, 'tp')
- vel_b_qkv: float32 [2, 12, 192], P(None, 'tp')
- vel_w_out: float32 [2, 768, 768], P(None, 'tp')
- vel_w_up: float32 [2, 768, 3072], P(None, None, 'tp')
- vel_b_up: float32 [2, 3072], P(None, 'tp')
- vel_w_down: float32 [2, 3072, 768], P(None, 'tp')
Outputs:
- output 1: float32 [], replicated
- output 2: float32 [50304, 768], P('tp')
- output 3: float32 [16, 768], replicated
- output 4: float32 [2, 768, 2304], P(None, None, 'tp')
- output 5: float32 [2, 12, 192], P(None, 'tp')
- output 6: float32 [2, 768, 768], P(None, 'tp')
- output 7: float32 [2, 768, 3072], P(None, None, 'tp')
- output 8: float32 [2, 3072], P(None, 'tp')
- output 9: float32 [2, 3072, 768], P(None, 'tp')
- output 10: float32 [50304, 768], P('tp')
- output 11: float32 [16, 768], replicated
- output 12: float32 [2, 768, 2304], P(None, None, 'tp')
- output 13: float32 [2, 12, 192], P(None, 'tp')
- output 14: float32 [2, 768, 768], P(None, 'tp')
- output 15: float32 [2, 768, 3072], P(None, None, 'tp')
- output 16: float32 [2, 3072], P(None, 'tp')
- output 17: float32 [2, 3072, 768], P(None, 'tp')
- output 18: float32 [50304, 768], P('tp')
- output 19: float32 [16, 768], replicated
- output 20: float32 [2, 768, 2304], P(None, None, 'tp')
- output 21: float32 [2, 12, 192], P(None, 'tp')
- output 22: float32 [2, 768, 768], P(None, 'tp')
- output 23: float32 [2, 768, 3072], P(None, None, 'tp')
- output 24: float32 [2, 3072], P(None, 'tp')
- output 25: float32 [2, 3072, 768], P(None, 'tp')
- output 26: bfloat16 [50304, 768], P('tp')
- output 27: bfloat16 [16, 768], replicated
- output 28: bfloat16 [2, 768, 2304], P(None, None, 'tp')
- output 29: bfloat16 [2, 12, 192], P(None, 'tp')
- output 30: bfloat16 [2, 768, 768], P(None, 'tp')
- output 31: bfloat16 [2, 768, 3072], P(None, None, 'tp')
- output 32: bfloat16 [2, 3072], P(None, 'tp')
- output 33: bfloat16 [2, 3072, 768], P(None, 'tp')
All inputs are finite; a program needn't handle non-finite values.
Results may differ from the reference program's by a relative error of at most 0.001.
Values sent between devices are 32-bit elements.
A program may use at most 1.5 GiB of HBM per device.

```python
import math
import jax
import jax.numpy as jnp
from jax import lax

VOCAB = 50304
D = 768
HEADS = 12
HEAD = 64
LAYERS = 2
SEQ = 1024
BATCH = 8
STEP_COUNT = 10

FF_WIDTH = 4 * D
NUM_VECS = 4 + 6 * LAYERS
LN_EPS = 1e-5
CLIP_NORM = 1.0
BETA_ONE = 0.9
BETA_TWO = 0.95
ADAM_EPS = 1e-8
WEIGHT_DECAY = 0.1
LEARN_RATE = 1e-3
DECAYED = (True, False, True, False, True, True, False, True)
PARAM_NAMES = ('embedding', 'vec_params', 'w_qkv', 'b_qkv', 'w_out', 'w_up', 'b_up', 'w_down')


def alibi_slopes(heads):
    closest = 2 ** int(math.floor(math.log2(heads)))
    first_base = 2.0 ** (-8.0 / closest)
    slopes = [first_base ** (head_idx + 1) for head_idx in range(closest)]
    extra_base = 2.0 ** (-4.0 / closest)
    extra_count = min(closest, heads - closest)
    return slopes + [extra_base ** (2 * head_idx + 1) for head_idx in range(extra_count)]


def layer_norm(values, gain, bias):
    centred = values - jnp.mean(values, axis=-1, keepdims=True)
    variance = jnp.mean(centred * centred, axis=-1, keepdims=True)
    return centred * lax.rsqrt(variance + LN_EPS) * gain + bias


def snap_bf16(values):
    return values + lax.stop_gradient(values.astype(jnp.bfloat16).astype(jnp.float32) - values)


def adam_update(master, grad_arr, moment, velocity, decayed):
    mom_new = BETA_ONE * moment + (1.0 - BETA_ONE) * grad_arr
    vel_new = BETA_TWO * velocity + (1.0 - BETA_TWO) * grad_arr * grad_arr
    mom_hat = mom_new / (1.0 - BETA_ONE ** STEP_COUNT)
    vel_hat = vel_new / (1.0 - BETA_TWO ** STEP_COUNT)
    direction = mom_hat / (jnp.sqrt(vel_hat) + ADAM_EPS)
    if decayed:
        direction = direction + WEIGHT_DECAY * master
    return master - LEARN_RATE * direction, mom_new, vel_new


def seq_loss(params, tok_seq, lab_seq):
    embedding, vec_params, w_qkv, b_qkv, w_out, w_up, b_up, w_down = params
    positions = jnp.arange(SEQ)
    rel_pos = (positions[None, :] - positions[:, None]).astype(jnp.float32)
    causal = positions[None, :] <= positions[:, None]
    slopes = jnp.array(alibi_slopes(HEADS), dtype=jnp.float32)
    emb_snap = snap_bf16(embedding)
    resid = layer_norm(jnp.take(emb_snap, tok_seq, axis=0), vec_params[0], vec_params[1])
    for layer in range(LAYERS):
        row_base = 2 + 6 * layer
        act_in = snap_bf16(layer_norm(resid, vec_params[row_base], vec_params[row_base + 1]))
        qkv = snap_bf16(jnp.dot(act_in, snap_bf16(w_qkv[layer]), preferred_element_type=jnp.float32) + b_qkv[layer].reshape(-1))
        qkv = qkv.reshape(SEQ, HEADS, 3, HEAD)
        scores = jnp.einsum('qhd,khd->hqk', qkv[:, :, 0], qkv[:, :, 1]) * HEAD ** -0.5 + slopes[:, None, None] * rel_pos[None]
        scores = jnp.where(causal[None], scores, -jnp.inf)
        probs = snap_bf16(jax.nn.softmax(scores, axis=-1))
        context = snap_bf16(jnp.einsum('hqk,khd->qhd', probs, qkv[:, :, 2])).reshape(SEQ, D)
        resid = resid + jnp.dot(context, snap_bf16(w_out[layer]), preferred_element_type=jnp.float32) + vec_params[row_base + 2]
        mlp_in = snap_bf16(layer_norm(resid, vec_params[row_base + 3], vec_params[row_base + 4]))
        hidden = snap_bf16(jax.nn.gelu(jnp.dot(mlp_in, snap_bf16(w_up[layer]), preferred_element_type=jnp.float32) + b_up[layer], approximate=True))
        resid = resid + jnp.dot(hidden, snap_bf16(w_down[layer]), preferred_element_type=jnp.float32) + vec_params[row_base + 5]
    final_row = 2 + 6 * LAYERS
    head_in = snap_bf16(layer_norm(resid, vec_params[final_row], vec_params[final_row + 1]))
    logits = jnp.dot(head_in, emb_snap.T, preferred_element_type=jnp.float32)
    target = jnp.take_along_axis(logits, lab_seq[:, None], axis=1)[:, 0]
    return jnp.sum(jax.nn.logsumexp(logits, axis=-1) - target)


def setup_inputs(seed: int = 0) -> dict:
    keys = jax.random.split(jax.random.key(seed), 28)
    tokens = jax.random.randint(keys[0], (BATCH, SEQ), 0, VOCAB, dtype=jnp.int32)
    label_flat = jax.random.randint(keys[1], (BATCH * SEQ,), 0, VOCAB, dtype=jnp.int32)
    spread = jnp.arange(8, dtype=jnp.int32) * (VOCAB // 8) + jax.random.randint(keys[2], (8,), 0, VOCAB // 8, dtype=jnp.int32)
    labels = label_flat.at[:8].set(spread).reshape(BATCH, SEQ)
    row_base = jnp.array([1.0, 0.0] + [1.0, 0.0, 0.0, 1.0, 0.0, 0.0] * LAYERS + [16.0, 0.0], dtype=jnp.float32)
    row_scale = jnp.array([0.2] * (2 + 6 * LAYERS) + [3.2, 0.5], dtype=jnp.float32)
    shapes = [(VOCAB, D), (NUM_VECS, D), (LAYERS, D, 3 * D), (LAYERS, HEADS, 3 * HEAD), (LAYERS, D, D), (LAYERS, D, FF_WIDTH), (LAYERS, FF_WIDTH), (LAYERS, FF_WIDTH, D)]
    scales = [0.2 * D ** -0.5, 1.0, D ** -0.5, 0.2, D ** -0.5, D ** -0.5, 0.2, FF_WIDTH ** -0.5]
    masters = [jax.random.normal(keys[3 + slot], shapes[slot], jnp.float32) * scales[slot] for slot in range(8)]
    masters[1] = row_base[:, None] + row_scale[:, None] * masters[1]
    grad_scale = float(VOCAB * D + NUM_VECS * D + LAYERS * (12 * D * D + 3 * D + FF_WIDTH)) ** -0.5
    moms = [jax.random.normal(keys[11 + slot], shapes[slot], jnp.float32) * grad_scale for slot in range(8)]
    vels = [jax.random.uniform(keys[19 + slot], shapes[slot], jnp.float32, 0.25, 2.0) * grad_scale ** 2 for slot in range(8)]
    result = {'tokens': tokens, 'labels': labels}
    for slot in range(8):
        result[PARAM_NAMES[slot]] = masters[slot]
    for slot in range(8):
        result['mom_' + PARAM_NAMES[slot]] = moms[slot]
    for slot in range(8):
        result['vel_' + PARAM_NAMES[slot]] = vels[slot]
    return result


def reference(tokens, labels, embedding, vec_params, w_qkv, b_qkv, w_out, w_up, b_up, w_down, mom_embedding, mom_vec_params, mom_w_qkv, mom_b_qkv, mom_w_out, mom_w_up, mom_b_up, mom_w_down, vel_embedding, vel_vec_params, vel_w_qkv, vel_b_qkv, vel_w_out, vel_w_up, vel_b_up, vel_w_down):
    masters = (embedding, vec_params, w_qkv, b_qkv, w_out, w_up, b_up, w_down)
    moms = (mom_embedding, mom_vec_params, mom_w_qkv, mom_b_qkv, mom_w_out, mom_w_up, mom_b_up, mom_w_down)
    vels = (vel_embedding, vel_vec_params, vel_w_qkv, vel_b_qkv, vel_w_out, vel_w_up, vel_b_up, vel_w_down)

    def total_loss(params):
        def one_seq(pair):
            return seq_loss(params, pair[0], pair[1])
        per_seq = lax.map(jax.checkpoint(one_seq), (tokens, labels))
        return jnp.sum(per_seq) / (BATCH * SEQ)

    loss, grads = jax.value_and_grad(total_loss)(masters)
    sq_total = sum(jnp.sum(grad_arr * grad_arr) for grad_arr in grads)
    clip_coef = jnp.minimum(1.0, CLIP_NORM / (jnp.sqrt(sq_total) + 1e-6))
    updated = [adam_update(masters[slot], grads[slot] * clip_coef, moms[slot], vels[slot], DECAYED[slot]) for slot in range(8)]
    new_masters = [entry[0] for entry in updated]
    new_moms = [entry[1] for entry in updated]
    new_vels = [entry[2] for entry in updated]
    new_bf16 = [entry.astype(jnp.bfloat16) for entry in new_masters]
    return (loss, *new_masters, *new_moms, *new_vels, *new_bf16)
```

```python
import functools
import math
import jax
import jax.numpy as jnp
from jax import lax
from jax.experimental import pallas as pl
from jax.experimental.pallas import tpu as pltpu
from jax.sharding import PartitionSpec as P

LN_EPS = 1e-5
CLIP_NORM = 1.0
BETA_ONE = 0.9
BETA_TWO = 0.95
ADAM_EPS = 1e-8
WEIGHT_DECAY = 0.1
LEARN_RATE = 1e-3
STEP_COUNT = 10
DECAYED = (True, False, True, False, True, True, False, True)
PARAM_SPECS = (P('tp', None), P(None, None), P(None, None, 'tp'), P(None, 'tp', None), P(None, 'tp', None), P(None, None, 'tp'), P(None, 'tp'), P(None, 'tp', None))
CONTRACT_ROWS = (((0,), (0,)), ((), ()))
CONTRACT_COLS = (((1,), (1,)), ((), ()))
F32 = jnp.float32
BF16 = jnp.bfloat16
ALL = ('tp', 'dp')
TP = 4
DP = 8
D = 768
SEQ = 1024
HEAD = 64
HEADS_LOC = 3
QW = HEADS_LOC * HEAD
QP = 256
FF_LOC = 768
LAYERS = 2
VOCAB_LOC = 12576
PIECE = 1576
PIECE_PAD = 1664
NTOK = 8192
QUART = 256
ATT_BLK = 256
HEAD_TILE = 512
NEG = -1e30
ROWS_QKV = 72
ROWS_OUT = 24
ROWS_FF = 96
PACK = 296


def alibi_slopes(heads):
    closest = 2 ** int(math.floor(math.log2(heads)))
    first_base = 2.0 ** (-8.0 / closest)
    slopes = [first_base ** (head_idx + 1) for head_idx in range(closest)]
    extra_base = 2.0 ** (-4.0 / closest)
    extra_count = min(closest, heads - closest)
    return slopes + [extra_base ** (2 * head_idx + 1) for head_idx in range(extra_count)]


def layer_norm(values, gain, bias):
    return normalise(values) * gain + bias


def normalise(values):
    centred = values - jnp.mean(values, axis=-1, keepdims=True)
    variance = jnp.mean(centred * centred, axis=-1, keepdims=True)
    return centred * lax.rsqrt(variance + LN_EPS)


def gelu_tanh(values):
    return jax.nn.gelu(values, approximate=True)


def adam_update(master, grad_arr, moment, velocity, decayed):
    mom_new = BETA_ONE * moment + (1.0 - BETA_ONE) * grad_arr
    vel_new = BETA_TWO * velocity + (1.0 - BETA_TWO) * grad_arr * grad_arr
    mom_hat = mom_new / (1.0 - BETA_ONE ** STEP_COUNT)
    vel_hat = vel_new / (1.0 - BETA_TWO ** STEP_COUNT)
    direction = mom_hat / (jnp.sqrt(vel_hat) + ADAM_EPS)
    if decayed:
        direction = direction + WEIGHT_DECAY * master
    return master - LEARN_RATE * direction, mom_new, vel_new


def dot(lhs, rhs, dims=(((1,), (0,)), ((), ()))):
    return lax.dot_general(lhs, rhs, dims, preferred_element_type=F32)


def unpack_kernel(which_ref, full_ref, qkv_ref, up_ref, down_ref, out_ref, bias_ref):
    del which_ref
    pairs = DP // 2
    up_at = ROWS_QKV
    down_at = up_at + ROWS_FF
    out_at = down_at + ROWS_FF
    bias_at = out_at + ROWS_OUT
    for pair in range(pairs):
        rows = pl.ds(2 * ROWS_OUT * pair, 2 * ROWS_OUT)
        for part in range(3):
            at = pl.ds(part * ROWS_OUT, ROWS_OUT)
            both = jnp.concatenate([full_ref[2 * pair, at, :], full_ref[2 * pair + 1, at, :]], axis=0)
            qkv_ref[0, part, rows, :] = both.astype(BF16)
        at = pl.ds(out_at, ROWS_OUT)
        both = jnp.concatenate([full_ref[2 * pair, at, :], full_ref[2 * pair + 1, at, :]], axis=0)
        out_ref[0, rows, :] = both.astype(BF16)
    zero = jnp.zeros((QP - QW, D), BF16)
    for part in range(3):
        qkv_ref[0, part, QW:, :] = zero
    out_ref[0, QW:, :] = zero
    for piece in range(DP):
        rows = pl.ds(ROWS_FF * piece, ROWS_FF)
        up_ref[rows, :] = full_ref[piece, pl.ds(up_at, ROWS_FF), :].astype(BF16)
        down_ref[rows, :] = full_ref[piece, pl.ds(down_at, ROWS_FF), :].astype(BF16)
    bias_ref[0] = full_ref[0, pl.ds(bias_at, 8), :]


def unpack_weights(full, core):
    grid_spec = pltpu.PrefetchScalarGridSpec(
        num_scalar_prefetch=1,
        grid=(2,),
        in_specs=[pl.BlockSpec((DP, PACK, D), lambda s, which: (2 * which[0] + s, 0, 0))],
        out_specs=[
            pl.BlockSpec((1, 3, QP, D), lambda s, which: (s, 0, 0, 0)),
            pl.BlockSpec((D, FF_LOC), lambda s, which: (0, s)),
            pl.BlockSpec((FF_LOC, D), lambda s, which: (s, 0)),
            pl.BlockSpec((1, QP, D), lambda s, which: (s, 0, 0)),
            pl.BlockSpec((1, 8, D), lambda s, which: (s, 0, 0)),
        ],
    )
    shapes = [
        jax.ShapeDtypeStruct((2, 3, QP, D), BF16),
        jax.ShapeDtypeStruct((D, 2 * FF_LOC), BF16),
        jax.ShapeDtypeStruct((2 * FF_LOC, D), BF16),
        jax.ShapeDtypeStruct((2, QP, D), BF16),
        jax.ShapeDtypeStruct((2, 8, D), F32),
    ]
    qkv, up, down, out, bias = pl.pallas_call(
        unpack_kernel,
        out_shape=shapes,
        grid_spec=grid_spec,
        compiler_params=pltpu.CompilerParams(vmem_limit_bytes=40 << 20),
        cost_estimate=pl.CostEstimate(flops=8 * 2368 * D * 2, bytes_accessed=22 << 20, transcendentals=0),
        name='unpack_weights',
    )(core.reshape(1), full)
    return qkv.reshape(2 * 3 * QP, D), up, down, out.reshape(2 * QP, D), bias


def pack_weights(w_qkv, b_qkv, w_out, w_up, b_up, w_down, dp_rank):
    qkv_t = w_qkv.T.reshape(HEADS_LOC, 3, HEAD, D).transpose(1, 0, 2, 3).reshape(3, QW, D)
    qkv_piece = lax.dynamic_slice(qkv_t, (0, dp_rank * ROWS_OUT, 0), (3, ROWS_OUT, D)).reshape(ROWS_QKV, D)
    up_piece = lax.dynamic_slice(w_up, (dp_rank * ROWS_FF, 0), (ROWS_FF, FF_LOC))
    down_piece = lax.dynamic_slice(w_down, (dp_rank * ROWS_FF, 0), (ROWS_FF, D))
    out_piece = lax.dynamic_slice(w_out, (dp_rank * ROWS_OUT, 0), (ROWS_OUT, D))
    b_row = b_qkv.reshape(HEADS_LOC, 3, HEAD).transpose(1, 0, 2).reshape(3, QW)
    b_row = jnp.pad(b_row, ((0, 0), (0, QP - QW))).reshape(1, D)
    bias = jnp.concatenate([b_row, b_up.reshape(1, FF_LOC), jnp.zeros((6, D), F32)], axis=0)
    return jnp.concatenate([qkv_piece, up_piece, down_piece, out_piece, bias], axis=0)


def head_masks(rows):
    lane = lax.broadcasted_iota(jnp.int32, (rows, QP), 1)
    return [(lane >= HEAD * j) & (lane < HEAD * (j + 1)) for j in range(HEADS_LOC)]


def block_probs(query, keys, slope, row0, width):
    scores = dot(query, keys, CONTRACT_COLS) * (HEAD ** -0.5)
    row = lax.broadcasted_iota(jnp.int32, (ATT_BLK, width), 0) + row0
    col = lax.broadcasted_iota(jnp.int32, (ATT_BLK, width), 1)
    rel = col - row
    scores = scores + slope * rel.astype(F32)
    scores = jnp.where(rel <= 0, scores, NEG)
    top = jnp.max(scores, axis=1, keepdims=True)
    shifted = jnp.exp(scores - top)
    return shifted * (1.0 / jnp.sum(shifted, axis=1, keepdims=True))


def attn_fwd_kernel(slope_ref, qkv_ref, ctx_ref):
    group = pl.program_id(0)
    masks = head_masks(ATT_BLK)
    for blk in range(SEQ // ATT_BLK):
        row0 = blk * ATT_BLK
        width = row0 + ATT_BLK
        query = qkv_ref[row0:width, 0:QP]
        keys = qkv_ref[0:width, QP:2 * QP]
        values = qkv_ref[0:width, 2 * QP:3 * QP]
        ctx = jnp.zeros((ATT_BLK, QP), F32)
        for j in range(HEADS_LOC):
            slope = slope_ref[group * HEADS_LOC + j]
            probs = block_probs(jnp.where(masks[j], query, 0).astype(BF16), keys, slope, row0, width)
            ctx = jnp.where(masks[j], dot(probs.astype(BF16), values), ctx)
        ctx_ref[row0:width, :] = ctx.astype(BF16)


def attn_bwd_kernel(slope_ref, qkv_ref, dctx_ref, dqkv_ref, dbias_ref, dk_ref, dv_ref):
    group = pl.program_id(0)
    masks = head_masks(ATT_BLK)
    dk_ref[...] = jnp.zeros_like(dk_ref)
    dv_ref[...] = jnp.zeros_like(dv_ref)
    dq_sum = jnp.zeros((1, QP), F32)
    for blk in range(SEQ // ATT_BLK):
        row0 = blk * ATT_BLK
        width = row0 + ATT_BLK
        query = qkv_ref[row0:width, 0:QP]
        keys = qkv_ref[0:width, QP:2 * QP]
        values = qkv_ref[0:width, 2 * QP:3 * QP]
        dctx = dctx_ref[row0:width, :]
        dq = jnp.zeros((ATT_BLK, QP), F32)
        for j in range(HEADS_LOC):
            slope = slope_ref[group * HEADS_LOC + j]
            q_one = jnp.where(masks[j], query, 0).astype(BF16)
            dc_one = jnp.where(masks[j], dctx, 0).astype(BF16)
            probs = block_probs(q_one, keys, slope, row0, width)
            d_probs = dot(dc_one, values, CONTRACT_COLS)
            inner = jnp.sum(probs * d_probs, axis=1, keepdims=True)
            d_scores = (probs * (d_probs - inner) * (HEAD ** -0.5)).astype(BF16)
            dv_ref[0:width, :] += dot(probs.astype(BF16), dc_one, CONTRACT_ROWS)
            dk_ref[0:width, :] += dot(d_scores, q_one, CONTRACT_ROWS)
            dq = jnp.where(masks[j], dot(d_scores, keys), dq)
        dqkv_ref[row0:width, 0:QP] = dq.astype(BF16)
        dq_sum = dq_sum + jnp.sum(dq, axis=0, keepdims=True)
    dqkv_ref[:, QP:2 * QP] = dk_ref[...].astype(BF16)
    dqkv_ref[:, 2 * QP:3 * QP] = dv_ref[...].astype(BF16)
    dbias_ref[0, :, 0:QP] = jnp.broadcast_to(dq_sum, (8, QP))
    dbias_ref[0, :, QP:2 * QP] = jnp.broadcast_to(jnp.sum(dk_ref[...], axis=0, keepdims=True), (8, QP))
    dbias_ref[0, :, 2 * QP:3 * QP] = jnp.broadcast_to(jnp.sum(dv_ref[...], axis=0, keepdims=True), (8, QP))


def attn_fwd(qkv, slopes):
    return pl.pallas_call(
        attn_fwd_kernel,
        grid=(2,),
        out_shape=jax.ShapeDtypeStruct((SEQ, 2 * QP), BF16),
        in_specs=[pl.BlockSpec(memory_space=pltpu.SMEM), pl.BlockSpec((SEQ, 3 * QP), lambda g: (0, g))],
        out_specs=pl.BlockSpec((SEQ, QP), lambda g: (0, g)),
        compiler_params=pltpu.CompilerParams(vmem_limit_bytes=40 << 20),
        cost_estimate=pl.CostEstimate(flops=10 * 1000 * 1000 * 1000, bytes_accessed=4 << 20, transcendentals=4 << 20),
        name='attn_fwd',
    )(slopes, qkv)


def attn_bwd(qkv, dctx, slopes):
    return pl.pallas_call(
        attn_bwd_kernel,
        grid=(2,),
        out_shape=[jax.ShapeDtypeStruct((SEQ, 6 * QP), BF16), jax.ShapeDtypeStruct((2, 8, 3 * QP), F32)],
        in_specs=[
            pl.BlockSpec(memory_space=pltpu.SMEM),
            pl.BlockSpec((SEQ, 3 * QP), lambda g: (0, g)),
            pl.BlockSpec((SEQ, QP), lambda g: (0, g)),
        ],
        out_specs=[pl.BlockSpec((SEQ, 3 * QP), lambda g: (0, g)), pl.BlockSpec((1, 8, 3 * QP), lambda g: (g, 0, 0))],
        scratch_shapes=[pltpu.VMEM((SEQ, QP), F32), pltpu.VMEM((SEQ, QP), F32)],
        compiler_params=pltpu.CompilerParams(vmem_limit_bytes=40 << 20),
        cost_estimate=pl.CostEstimate(flops=25 * 1000 * 1000 * 1000, bytes_accessed=8 << 20, transcendentals=4 << 20),
        name='attn_bwd',
    )(slopes, qkv, dctx)


ROW_CHUNK = 128
CHUNKS = PIECE_PAD // ROW_CHUNK


def head_fwd_kernel(valid_ref, xhat_ref, gain_ref, bias_ref, emb_ref, lab_ref, head_ref, logit_ref, stat_ref):
    head_in = (xhat_ref[...] * gain_ref[...] + bias_ref[...]).astype(BF16)
    head_ref[...] = head_in
    valid = valid_ref[0]
    top = jnp.full((1, HEAD_TILE), NEG, F32)
    for chunk in range(CHUNKS):
        rows = slice(chunk * ROW_CHUNK, (chunk + 1) * ROW_CHUNK)
        part = dot(emb_ref[rows, :], head_in, CONTRACT_COLS)
        if (chunk + 1) * ROW_CHUNK > PIECE - 32:
            row = lax.broadcasted_iota(jnp.int32, part.shape, 0) + chunk * ROW_CHUNK
            part = jnp.where(row < valid, part, NEG)
        logit_ref[rows, :] = part
        top = jnp.maximum(top, jnp.max(part, axis=0, keepdims=True))
    total = jnp.zeros((1, HEAD_TILE), F32)
    target = jnp.zeros((1, HEAD_TILE), F32)
    label = lab_ref[...]
    for chunk in range(CHUNKS):
        rows = slice(chunk * ROW_CHUNK, (chunk + 1) * ROW_CHUNK)
        part = logit_ref[rows, :]
        row = lax.broadcasted_iota(jnp.int32, part.shape, 0) + chunk * ROW_CHUNK
        total = total + jnp.sum(jnp.exp(part - top), axis=0, keepdims=True)
        target = target + jnp.sum(jnp.where(row == label, part, 0.0), axis=0, keepdims=True)
    stat_ref[0:1, :] = top
    stat_ref[1:2, :] = total
    stat_ref[2:3, :] = target
    stat_ref[3:8, :] = jnp.zeros((5, HEAD_TILE), F32)


def head_bwd_kernel(logit_ref, head_ref, emb_ref, lab_ref, stat_ref, dhead_ref, gemb_ref):
    @pl.when(pl.program_id(0) == 0)
    def _():
        gemb_ref[...] = jnp.zeros_like(gemb_ref)

    top = stat_ref[0:1, :]
    inverse = 1.0 / stat_ref[1:2, :]
    label = lab_ref[...]
    head_in = head_ref[...]
    dhead = jnp.zeros((HEAD_TILE, D), F32)
    for chunk in range(CHUNKS):
        rows = slice(chunk * ROW_CHUNK, (chunk + 1) * ROW_CHUNK)
        part = logit_ref[rows, :]
        row = lax.broadcasted_iota(jnp.int32, part.shape, 0) + chunk * ROW_CHUNK
        soft = jnp.exp(part - top) * inverse
        d_logit = ((soft - jnp.where(row == label, 1.0, 0.0)) * (1.0 / NTOK)).astype(BF16)
        gemb_ref[rows, :] += dot(d_logit, head_in)
        dhead = dhead + dot(d_logit, emb_ref[rows, :], CONTRACT_ROWS)
    dhead_ref[...] = dhead


def head_fwd(xhat, gain, bias, emb_piece, label_row, valid):
    return pl.pallas_call(
        head_fwd_kernel,
        grid=(NTOK // HEAD_TILE,),
        out_shape=[
            jax.ShapeDtypeStruct((NTOK, D), BF16),
            jax.ShapeDtypeStruct((PIECE_PAD, NTOK), F32),
            jax.ShapeDtypeStruct((8, NTOK), F32),
        ],
        in_specs=[
            pl.BlockSpec(memory_space=pltpu.SMEM),
            pl.BlockSpec((HEAD_TILE, D), lambda t: (t, 0)),
            pl.BlockSpec((1, D), lambda t: (0, 0)),
            pl.BlockSpec((1, D), lambda t: (0, 0)),
            pl.BlockSpec((PIECE_PAD, D), lambda t: (0, 0)),
            pl.BlockSpec((1, HEAD_TILE), lambda t: (0, t)),
        ],
        out_specs=[
            pl.BlockSpec((HEAD_TILE, D), lambda t: (t, 0)),
            pl.BlockSpec((PIECE_PAD, HEAD_TILE), lambda t: (0, t)),
            pl.BlockSpec((8, HEAD_TILE), lambda t: (0, t)),
        ],
        compiler_params=pltpu.CompilerParams(vmem_limit_bytes=48 << 20),
        cost_estimate=pl.CostEstimate(flops=2 * NTOK * PIECE_PAD * D, bytes_accessed=96 << 20, transcendentals=NTOK * PIECE_PAD),
        name='head_fwd',
    )(valid.reshape(1), xhat, gain, bias, emb_piece, label_row)


def head_bwd(logits, head_in, emb_piece, label_row, stats):
    return pl.pallas_call(
        head_bwd_kernel,
        grid=(NTOK // HEAD_TILE,),
        out_shape=[jax.ShapeDtypeStruct((NTOK, D), F32), jax.ShapeDtypeStruct((PIECE_PAD, D), F32)],
        in_specs=[
            pl.BlockSpec((PIECE_PAD, HEAD_TILE), lambda t: (0, t)),
            pl.BlockSpec((HEAD_TILE, D), lambda t: (t, 0)),
            pl.BlockSpec((PIECE_PAD, D), lambda t: (0, 0)),
            pl.BlockSpec((1, HEAD_TILE), lambda t: (0, t)),
            pl.BlockSpec((8, HEAD_TILE), lambda t: (0, t)),
        ],
        out_specs=[pl.BlockSpec((HEAD_TILE, D), lambda t: (t, 0)), pl.BlockSpec((PIECE_PAD, D), lambda t: (0, 0))],
        compiler_params=pltpu.CompilerParams(vmem_limit_bytes=48 << 20),
        cost_estimate=pl.CostEstimate(flops=4 * NTOK * PIECE_PAD * D, bytes_accessed=96 << 20, transcendentals=NTOK * PIECE_PAD),
        name='head_bwd',
    )(logits, head_in, emb_piece, label_row, stats)


def partner_core(values):
    return lax.ppermute(values, 'dp', [(rank, rank ^ 1) for rank in range(DP)])


def line_pairs(flip):
    return [(z * DP + rank, (z ^ flip) * DP + rank) for z in range(TP) for rank in range(DP)]


def join_core(partial):
    return partial + partner_core(partial)


def device_step(tokens, labels, *state):
    masters = state[0:8]
    moms = state[8:16]
    vels = state[16:24]
    embedding, vec_params, w_qkv, b_qkv, w_out, w_up, b_up, w_down = masters
    z_rank = lax.axis_index('tp')
    dp_rank = lax.axis_index('dp')
    core = dp_rank % 2
    parity = z_rank % 2
    high = z_rank // 2
    quarter = high * 2 + core
    own_shard = parity
    is_holder = core == high

    slope_all = jnp.array(alibi_slopes(HEADS_LOC * TP), dtype=F32)
    slopes = lax.dynamic_slice_in_dim(slope_all, core * 2 * HEADS_LOC, 2 * HEADS_LOC)

    id_local = tokens.reshape(-1) - z_rank * VOCAB_LOC
    in_shard = (id_local >= 0) & (id_local < VOCAB_LOC)
    safe_ids = jnp.clip(id_local, 0, VOCAB_LOC - 1)
    picked = lax.reduce_precision(jnp.take(embedding, safe_ids, axis=0), 8, 7)
    x_own = lax.psum(jnp.where(in_shard[:, None], picked, 0.0), 'tp')

    full = [lax.all_gather(pack_weights(w_qkv[l], b_qkv[l], w_out[l], w_up[l], b_up[l], w_down[l], dp_rank), ALL) for l in range(LAYERS)]
    ids_all = lax.all_gather(jnp.concatenate([tokens, labels], axis=0), 'dp')

    pairs = [(z * DP + 2 * k + z % 2, z * DP + 2 * k + 1 - z % 2) for z in range(TP) for k in range(DP // 2)]
    x_other = lax.ppermute(x_own, ALL, pairs)
    x_embed = jnp.where(core == parity, x_own, x_other)
    resid, ln_zero_vjp = jax.vjp(layer_norm, x_embed, vec_params[0], vec_params[1])

    weights = []
    saved = []
    for layer in range(LAYERS):
        row_base = 2 + 6 * layer
        qkv_w, up_w, down_w, out_w, biases = unpack_weights(full[layer], core)
        normed_one, ln_one_vjp = jax.vjp(layer_norm, resid, vec_params[row_base], vec_params[row_base + 1])
        act_in = normed_one.astype(BF16)
        qkv = (dot(act_in, qkv_w, CONTRACT_COLS) + biases[:, 0].reshape(-1)).astype(BF16)
        context = attn_fwd(qkv, slopes)
        mid = resid + join_core(dot(context, out_w)) + vec_params[row_base + 2]
        normed_two, ln_two_vjp = jax.vjp(layer_norm, mid, vec_params[row_base + 3], vec_params[row_base + 4])
        mlp_in = normed_two.astype(BF16)
        pre_act = dot(mlp_in, up_w) + biases[:, 1].reshape(-1)
        act_out, gelu_vjp = jax.vjp(gelu_tanh, pre_act)
        hidden = act_out.astype(BF16)
        resid = mid + join_core(dot(hidden, down_w)) + vec_params[row_base + 5]
        weights.append((qkv_w, up_w, down_w, out_w))
        saved.append((ln_one_vjp, act_in, qkv, context, ln_two_vjp, mlp_in, gelu_vjp, hidden))

    final_row = 2 + 6 * LAYERS
    normed_fin, ln_fin_vjp = jax.vjp(layer_norm, resid, vec_params[final_row], vec_params[final_row + 1])
    del normed_fin
    xhat = lax.dynamic_slice_in_dim(normalise(resid), quarter * QUART, QUART)
    xhat_all = lax.all_gather(xhat, ALL, tiled=True)

    def gathered_order(ids):
        return ids.reshape(DP // 2, 2, 2, 2, QUART).transpose(2, 1, 0, 3, 4).reshape(-1)

    token_all = gathered_order(ids_all[:, 0])
    label_all = gathered_order(ids_all[:, 1])
    valid = jnp.minimum(PIECE, VOCAB_LOC - dp_rank * PIECE)
    piece_start = jnp.minimum(dp_rank * PIECE, VOCAB_LOC - PIECE)
    emb_piece = lax.dynamic_slice_in_dim(embedding, piece_start, PIECE).astype(BF16)
    over = DP * PIECE - VOCAB_LOC
    emb_piece = jnp.where(dp_rank == DP - 1, jnp.roll(emb_piece, -over, axis=0), emb_piece)
    emb_piece = jnp.pad(emb_piece, ((0, PIECE_PAD - PIECE), (0, 0)))
    label_row = (label_all - z_rank * VOCAB_LOC - dp_rank * PIECE)
    label_row = jnp.where(label_row < valid, label_row, -1).reshape(1, NTOK)
    head_in, logits, stat_loc = head_fwd(xhat_all, vec_params[final_row:final_row + 1], vec_params[final_row + 1:final_row + 2], emb_piece, label_row, valid)
    glob_max = lax.pmax(stat_loc[0], ALL)
    sums = lax.psum(jnp.stack([stat_loc[1] * jnp.exp(stat_loc[0] - glob_max), stat_loc[2]]), ALL)
    loss = jnp.sum(glob_max + jnp.log(sums[0]) - sums[1]) / NTOK
    stats = jnp.concatenate([glob_max[None], sums[0:1], jnp.zeros((6, NTOK), F32)], axis=0)
    d_head_part, g_piece = head_bwd(logits, head_in, emb_piece, label_row, stats)
    d_quart = lax.psum_scatter(d_head_part, ALL, scatter_dimension=0, tiled=True)
    d_far = lax.ppermute(d_quart, ALL, line_pairs(2))
    mine = jnp.where(high == 0, jnp.stack([d_quart, d_far]), jnp.stack([d_far, d_quart]))
    theirs = partner_core(mine)
    d_head = jnp.where(core == 0, jnp.stack([mine, theirs], axis=1), jnp.stack([theirs, mine], axis=1)).reshape(SEQ, D)
    g_head = lax.all_gather(g_piece[:PIECE], 'dp', tiled=True)

    vec_grads = {}
    d_resid, vec_grads[final_row], vec_grads[final_row + 1] = ln_fin_vjp(d_head)
    layer_grads = {}
    bias_grads = {}
    for layer in reversed(range(LAYERS)):
        ln_one_vjp, act_in, qkv, context, ln_two_vjp, mlp_in, gelu_vjp, hidden = saved[layer]
        qkv_w, up_w, down_w, out_w = weights[layer]
        row_base = 2 + 6 * layer
        vec_grads[row_base + 5] = jnp.sum(d_resid, axis=0)
        d_out = d_resid.astype(BF16)
        d_hidden = dot(d_out, down_w, CONTRACT_COLS)
        d_pre = gelu_vjp(d_hidden)[0]
        g_bup = jnp.sum(d_pre, axis=0)
        d_pre_b = d_pre.astype(BF16)
        d_norm_two = join_core(dot(d_pre_b, up_w, CONTRACT_COLS))
        d_mid_ln, vec_grads[row_base + 3], vec_grads[row_base + 4] = ln_two_vjp(d_norm_two)
        d_mid = d_resid + d_mid_ln
        vec_grads[row_base + 2] = jnp.sum(d_mid, axis=0)
        d_attn = d_mid.astype(BF16)
        d_context = dot(d_attn, out_w, CONTRACT_COLS).astype(BF16)
        d_qkv, g_bqkv = attn_bwd(qkv, d_context, slopes)
        d_norm_one = join_core(dot(d_qkv, qkv_w))
        d_res_ln, vec_grads[row_base], vec_grads[row_base + 1] = ln_one_vjp(d_norm_one)
        d_resid = d_mid + d_res_ln
        bias_grads[layer] = jnp.stack([g_bqkv[:, 0], g_bup.reshape(2, FF_LOC)], axis=1)

        def weight_grads(shard):
            d_pre_s = lax.dynamic_slice_in_dim(d_pre_b, shard * FF_LOC, FF_LOC, axis=1)
            hidden_s = lax.dynamic_slice_in_dim(hidden, shard * FF_LOC, FF_LOC, axis=1)
            context_s = lax.dynamic_slice_in_dim(context, shard * QP, QP, axis=1)
            d_qkv_s = lax.dynamic_slice_in_dim(d_qkv, shard * 3 * QP, 3 * QP, axis=1)
            g_qkv = dot(d_qkv_s, act_in, CONTRACT_ROWS).reshape(3, QP, D)[:, :QW].reshape(3 * QW, D)
            g_out = dot(context_s, d_attn, CONTRACT_ROWS)[:QW]
            return g_qkv, g_out, dot(mlp_in, d_pre_s, CONTRACT_ROWS), dot(hidden_s, d_out, CONTRACT_ROWS)

        kept = weight_grads(own_shard)
        sent = weight_grads(1 - own_shard)
        cross = [(z * DP + 2 * k + z // 2, (z ^ 1) * DP + 2 * k + 1 - z // 2) for z in range(TP) for k in range(DP // 2)]
        total = [jnp.where(is_holder, keep, lax.ppermute(send, ALL, cross)) for keep, send in zip(kept, sent)]
        layer_grads[layer] = lax.psum(tuple(total), 'dp')
    d_embed, vec_grads[0], vec_grads[1] = ln_zero_vjp(d_resid)

    counted = (z_rank < 2).astype(F32)
    bias_stack = jnp.stack([bias_grads[layer] for layer in range(LAYERS)], axis=1) * counted
    bias_slots = lax.dynamic_update_slice(jnp.zeros((TP, LAYERS, 2, D), F32), bias_stack, (2 * core, 0, 0, 0))
    vec_stack = jnp.stack([vec_grads[row] for row in range(final_row + 2)]) * (counted * (core == 0))
    small = lax.psum(jnp.concatenate([vec_stack, bias_slots.reshape(TP * LAYERS * 2, D)], axis=0), ALL)
    g_vec = small[:final_row + 2]
    g_bias = lax.dynamic_index_in_dim(small[final_row + 2:].reshape(TP, LAYERS, 2, D), z_rank, keepdims=False)
    g_bqkv = g_bias[:, 0].reshape(LAYERS, 3, QP)[:, :, :QW].reshape(LAYERS, 3, HEADS_LOC, HEAD).transpose(0, 2, 1, 3).reshape(LAYERS, HEADS_LOC, 3 * HEAD)
    g_bup = g_bias[:, 1]

    d_quart_embed = lax.dynamic_slice_in_dim(d_embed, quarter * QUART, QUART)
    d_rows = lax.all_gather(d_quart_embed, ALL, tiled=True)
    row_ids = token_all - z_rank * VOCAB_LOC
    row_ids = jnp.where((row_ids >= 0) & (row_ids < VOCAB_LOC), row_ids, DP * PIECE)
    g_emb = g_head.at[row_ids].add(d_rows, mode='drop')[:VOCAB_LOC]

    def stacked(slot):
        return [layer_grads[layer][slot] for layer in range(LAYERS)]

    g_qkv = jnp.stack([g.reshape(3, HEADS_LOC, HEAD, D).transpose(3, 1, 0, 2).reshape(D, 3 * QW) for g in stacked(0)])
    grads = [g_emb, g_vec, g_qkv, g_bqkv, jnp.stack(stacked(1)), jnp.stack(stacked(2)), g_bup, jnp.stack(stacked(3))]

    sq_sharded = sum(jnp.sum(grads[slot] * grads[slot]) for slot in range(8) if slot != 1)
    sq_total = lax.psum(sq_sharded, 'tp') + jnp.sum(g_vec * g_vec)
    clip_coef = jnp.minimum(1.0, CLIP_NORM / (jnp.sqrt(sq_total) + 1e-6))
    updated = [adam_update(masters[slot], grads[slot] * clip_coef, moms[slot], vels[slot], DECAYED[slot]) for slot in range(8)]
    new_masters = [entry[0] for entry in updated]
    new_moms = [entry[1] for entry in updated]
    new_vels = [entry[2] for entry in updated]
    new_bf16 = [entry.astype(BF16) for entry in new_masters]
    return (loss, *new_masters, *new_moms, *new_vels, *new_bf16)


def solution(mesh):
    data_spec = P('dp', None)
    return jax.shard_map(device_step, mesh=mesh, in_specs=(data_spec, data_spec) + PARAM_SPECS * 3, out_specs=(P(),) + PARAM_SPECS * 4, check_vma=False)
```
